32 devices in a mesh: pb: 8 (over z, core), sp: 4 (over y, x).
Axes of the slice: x: 2, y: 2, z: 4, core: 2. Of those that a mesh axis runs over, the one named last changes fastest.
Arguments:
- nodes: bfloat16 [8192, 1024], P(('pb', 'sp')), may hold values from -40 to 40
- project_in: bfloat16 [1024, 3072], replicated, may hold values from -0.3 to 0.3
- project_out: bfloat16 [1024, 1024], replicated, may hold values from -0.1875 to 0.1875
- tile_list: int32 [64, 32], replicated, may hold values from 0 to 63, as said below
- tile_count: int32 [64], replicated, may hold values from 2 to 32, as said below
Outputs:
- mixed: bfloat16 [8192, 1024], P(('pb', 'sp'))
The draws below stay inside these ranges and needn't reach their ends.
Inputs may be any that keep to these rules, and one draw needn't show every extreme that they name: `tile_list`: position 0 of row t is t itself. Over the live positions of the rows of one group (rows g * 8 to (g + 1) * 8 - 1), at most 4 distinct tiles of any other group are listed, and exactly 4 of the next group's tiles (group g + 1, after the last comes the first). A tile may stand more than once in a row. `tile_count`: row 0 has 32.
All inputs are finite; a program needn't handle non-finite values.
Results may differ from the reference program's by a relative error of at most 0.0082.
Values may be sent and summed in bfloat16 or wider, within the bound.
A program may use at most 128 MiB of HBM per device.

```python
import jax
import jax.numpy as jnp
from jax import lax

D = 1024
HEADS = 16
HEAD_DIM = 64
TILE = 128
LISTED = 32
SLOTS = 4
GROUP_TILES = 8
TILES = 64
NODES = 8192


def draw_nodes(key, part):
    keys = jax.random.split(key, 1)
    base = jnp.clip(jax.random.normal(keys[0], (NODES, D), jnp.float32), -6.0, 6.0)
    values_out = base
    return values_out.astype(jnp.bfloat16)


def draw_project_in(key, part):
    fresh = jnp.clip(jax.random.normal(key, (D, HEADS, 3, HEAD_DIM), jnp.float32), -6.0, 6.0) * D ** (-0.5)
    fresh = jnp.clip(fresh, -0.296875, 0.296875)
    return fresh.reshape(D, 3 * D).astype(jnp.bfloat16)


def draw_tile_list(key, part):
    keys = jax.random.split(key, 5)
    groups = TILES // GROUP_TILES
    tile_ids = jnp.arange(TILES, dtype=jnp.int32)
    group_of = tile_ids // GROUP_TILES
    local_of = tile_ids % GROUP_TILES
    pool_base = jax.random.randint(keys[0], (groups, groups), 0, GROUP_TILES, dtype=jnp.int32)
    kinds = jax.random.randint(keys[1], (TILES, LISTED), 0, 4, dtype=jnp.int32)
    offsets = jax.random.randint(keys[2], (TILES, LISTED), -4, 5, dtype=jnp.int32)
    hops = jax.random.randint(keys[3], (TILES, LISTED), 1, groups, dtype=jnp.int32)
    picks = jax.random.randint(keys[4], (TILES, LISTED), 0, SLOTS, dtype=jnp.int32)
    nearby = group_of[:, None] * GROUP_TILES + (local_of[:, None] + offsets) % GROUP_TILES
    owners = (group_of[:, None] + hops) % groups
    faraway = owners * GROUP_TILES + (pool_base[group_of[:, None], owners] + picks) % GROUP_TILES
    entries = jnp.where(kinds == 3, faraway, nearby)
    next_owner = (group_of + 1) % groups
    forced = next_owner * GROUP_TILES + (pool_base[group_of, next_owner] + local_of % SLOTS) % GROUP_TILES
    columns = jnp.arange(LISTED, dtype=jnp.int32)[None, :]
    entries = jnp.where(columns == 0, tile_ids[:, None], jnp.where(columns == 1, forced[:, None], entries))
    return entries.astype(jnp.int32)


def draw_tile_count(key, part):
    keys = jax.random.split(key, 2)
    groups = TILES // GROUP_TILES
    tile_ids = jnp.arange(TILES, dtype=jnp.int32)
    row_draw = jax.random.randint(keys[0], (TILES,), 0, 31, dtype=jnp.int32)
    group_draw = jax.random.randint(keys[1], (groups,), 15, 31, dtype=jnp.int32)
    counts = 2 + row_draw * group_draw[tile_ids // GROUP_TILES] * (LISTED - 2) // 900
    counts = jnp.where(tile_ids == 0, LISTED, counts)
    return counts.astype(jnp.int32)


def normal_values(stream_key, dims, scale, reach, held_as=jnp.bfloat16):
    drawn = scale * jax.random.normal(stream_key, dims, jnp.float32)
    return jnp.clip(drawn, min=-reach, max=reach).astype(held_as)


def setup_inputs(seed: int = 0) -> dict:
    streams_of = jax.random.split(jax.random.key(seed), 6)
    return {
        "nodes": draw_nodes(jax.random.fold_in(streams_of[5], 71), 0),
        "project_in": draw_project_in(jax.random.fold_in(streams_of[5], 71), 0),
        "project_out": normal_values(streams_of[2], (D, D), D ** -0.5, 0.1875),
        "tile_list": draw_tile_list(jax.random.fold_in(streams_of[5], 71), 0),
        "tile_count": draw_tile_count(jax.random.fold_in(streams_of[5], 71), 0),
    }


NEGATIVE = -1.0e30


def live_mask(tile_list, tile_count):
    listed = tile_list.shape[1]
    places = jnp.arange(listed, dtype=jnp.int32)
    inside = places[None, :] < tile_count[:, None]
    earlier = (places[:, None] > places[None, :])[None, :, :]
    repeats = (tile_list[:, :, None] == tile_list[:, None, :]) & earlier
    return inside & jnp.logical_not(jnp.any(repeats, axis=2))


def reference(nodes, project_in, project_out, tile_list, tile_count):
    all_tiles = tile_list.shape[0]
    node_tiles = nodes.reshape(all_tiles, TILE, D)

    def project_tile(block_nodes):
        return jnp.dot(block_nodes, project_in, preferred_element_type=jnp.float32).astype(jnp.bfloat16)

    projected = lax.map(project_tile, node_tiles).reshape(all_tiles, TILE, HEADS, 3, HEAD_DIM)
    queries = projected[:, :, :, 0]
    keys_all = projected[:, :, :, 1]
    values_all = projected[:, :, :, 2]
    usable = live_mask(tile_list, tile_count)
    score_scale = HEAD_DIM ** -0.5

    def attend_tile(packed):
        query_tile, chosen, allowed = packed
        fetched_keys = keys_all[chosen].astype(jnp.float32)
        fetched_values = values_all[chosen].astype(jnp.float32)
        scores = jnp.einsum("bhe,jkhe->hbjk", query_tile.astype(jnp.float32), fetched_keys) * score_scale
        allowed_mask = allowed[None, None, :, None]
        scores = jnp.where(allowed_mask, scores, NEGATIVE)
        highest = jnp.max(scores, axis=(2, 3), keepdims=True)
        weights = jnp.where(allowed_mask, jnp.exp(scores - highest), 0.0)
        running_total = jnp.sum(weights, axis=(2, 3))
        rounded = lax.optimization_barrier(weights.astype(jnp.bfloat16)).astype(jnp.float32)
        summed = jnp.einsum("hbjk,jkhe->bhe", rounded, fetched_values)
        return (summed / jnp.transpose(running_total)[:, :, None]).astype(jnp.bfloat16)

    attended = lax.map(attend_tile, (queries, tile_list, usable)).reshape(all_tiles, TILE, D)

    def finish_tile(packed):
        node_block, attended_block = packed
        added = node_block.astype(jnp.float32) + jnp.dot(attended_block, project_out, preferred_element_type=jnp.float32)
        return added.astype(jnp.bfloat16)

    mixed_out = lax.map(finish_tile, (node_tiles, attended)).reshape(NODES, D)
    return mixed_out
```

```python
import functools

import jax
import jax.numpy as jnp
from jax import lax
from jax.experimental import pallas as pl
from jax.experimental.pallas import tpu as pltpu
from jax.sharding import PartitionSpec as P

HEADS = 16
HEAD_DIM = 64
TILE = 128
PAIR = 2 * HEAD_DIM
PAIRS = HEADS // 2
NEGATIVE = -1e30
TRANSPOSED = (((1,), (1,)), ((), ()))
VMEM_LIMIT = 60 * 1024 * 1024


def query_kernel(x_ref, wq_ref, q_ref):
    q = lax.dot_general(wq_ref[...], x_ref[...], TRANSPOSED, preferred_element_type=jnp.float32)
    q = q.astype(jnp.bfloat16) * jnp.bfloat16(HEAD_DIM ** -0.5)
    for j in range(q_ref.shape[0]):
        q_ref[j] = q[:, j * TILE : (j + 1) * TILE]


def key_value_kernel(x_ref, wk_ref, wv_ref, k_ref, v_ref):
    x = x_ref[...]
    k = lax.dot_general(x, wk_ref[...], TRANSPOSED, preferred_element_type=jnp.float32)
    v = lax.dot_general(wv_ref[...], x, TRANSPOSED, preferred_element_type=jnp.float32)
    k_ref[...] = k.astype(jnp.bfloat16)
    v = v.astype(jnp.bfloat16)
    for j in range(v_ref.shape[0]):
        v_ref[j] = v[:, j * TILE : (j + 1) * TILE]


def project_query(x, wq):
    rows, width = x.shape
    return pl.pallas_call(
        query_kernel,
        out_shape=jax.ShapeDtypeStruct((rows // TILE, width, TILE), jnp.bfloat16),
        compiler_params=pltpu.CompilerParams(vmem_limit_bytes=VMEM_LIMIT),
        cost_estimate=pl.CostEstimate(flops=2 * rows * width * width, bytes_accessed=2 * width * width, transcendentals=0),
        name="query",
    )(x, wq)


def project_key_value(x, wk, wv, step):
    rows, width = x.shape
    return pl.pallas_call(
        key_value_kernel,
        grid=(rows // step,),
        in_specs=[
            pl.BlockSpec((step, width), lambda i: (i, 0)),
            pl.BlockSpec((width, width), lambda i: (0, 0)),
            pl.BlockSpec((width, width), lambda i: (0, 0)),
        ],
        out_specs=[
            pl.BlockSpec((step, width), lambda i: (i, 0)),
            pl.BlockSpec((step // TILE, width, TILE), lambda i: (i, 0, 0)),
        ],
        out_shape=[
            jax.ShapeDtypeStruct((rows, width), jnp.bfloat16),
            jax.ShapeDtypeStruct((rows // TILE, width, TILE), jnp.bfloat16),
        ],
        compiler_params=pltpu.CompilerParams(vmem_limit_bytes=VMEM_LIMIT),
        cost_estimate=pl.CostEstimate(
            flops=4 * rows * width * width, bytes_accessed=6 * rows * width + 4 * width * width, transcendentals=0
        ),
        name="key_value",
    )(x, wk, wv)


def attend_kernel(first, key_tiles, flags, q_ref, k_ref, v_ref, *rest):
    if first:
        acc_ref, m_ref, l_ref, spread = rest
    else:
        acc_in, m_in, l_in, out_ref, stat_ref, spread, acc_ref, m_ref, l_ref = rest
    tile = pl.program_id(0)

    @pl.when(tile == 0)
    def _():
        spread[...] = jnp.zeros_like(spread)

    for p in range(PAIRS):
        low = p * PAIR
        spread[p, :HEAD_DIM, :TILE] = q_ref[0, low : low + HEAD_DIM, :]
        spread[p, HEAD_DIM:, TILE:] = q_ref[0, low + HEAD_DIM : low + PAIR, :]
    if first:
        acc_ref[...] = jnp.zeros_like(acc_ref)
        m_ref[...] = jnp.full_like(m_ref, NEGATIVE)
        l_ref[...] = jnp.zeros_like(l_ref)
    else:
        acc_ref[...] = acc_in[...]
        m_ref[...] = m_in[...]
        l_ref[...] = l_in[...]

    def visit(kt, carry):
        @pl.when(flags[tile * key_tiles + kt] > 0)
        def _():
            rows = pl.ds(pl.multiple_of(kt * TILE, TILE), TILE)
            for p in range(PAIRS):
                low = p * PAIR
                s = jnp.dot(k_ref[rows, low : low + PAIR], spread[p], preferred_element_type=jnp.float32)
                m_old = m_ref[0, p : p + 1, :]
                m_new = jnp.maximum(m_old, jnp.max(s, axis=0, keepdims=True))
                fade = jnp.exp(m_old - m_new)
                w = jnp.exp(s - m_new)
                m_ref[0, p : p + 1, :] = m_new
                l_ref[0, p : p + 1, :] = l_ref[0, p : p + 1, :] * fade + jnp.sum(w, axis=0, keepdims=True)
                w = w.astype(jnp.bfloat16)
                for i in range(2):
                    at = low + i * HEAD_DIM
                    half = slice(i * TILE, (i + 1) * TILE)
                    o = jnp.dot(v_ref[kt, at : at + HEAD_DIM, :], w[:, half], preferred_element_type=jnp.float32)
                    acc_ref[0, at : at + HEAD_DIM, :] = acc_ref[0, at : at + HEAD_DIM, :] * fade[:, half] + o

        return carry

    lax.fori_loop(0, key_tiles, visit, 0)
    if not first:
        total = l_ref[0]
        inverse = jnp.where(total > 0.0, 1.0 / jnp.where(total > 0.0, total, 1.0), 0.0)
        for h in range(HEADS):
            half = slice((h % 2) * TILE, (h % 2 + 1) * TILE)
            at = h * HEAD_DIM
            scaled = acc_ref[0, at : at + HEAD_DIM, :] * inverse[h // 2 : h // 2 + 1, half]
            out_ref[0, at : at + HEAD_DIM, :] = scaled.astype(jnp.bfloat16)
        stat_ref[0, 0] = m_ref[0]
        stat_ref[0, 1] = total


def attend(flags, q, k, v, state=None):
    tiles, width, _ = q.shape
    key_tiles = v.shape[0]
    first = state is None
    per_tile = lambda *shape: pl.BlockSpec((1,) + shape, lambda t, f: (t,) + (0,) * len(shape))
    whole = lambda *shape: pl.BlockSpec(shape, lambda t, f: (0,) * len(shape))
    state_specs = [per_tile(width, TILE), per_tile(PAIRS, 2 * TILE), per_tile(PAIRS, 2 * TILE)]
    state_shapes = [
        jax.ShapeDtypeStruct((tiles, width, TILE), jnp.float32),
        jax.ShapeDtypeStruct((tiles, PAIRS, 2 * TILE), jnp.float32),
        jax.ShapeDtypeStruct((tiles, PAIRS, 2 * TILE), jnp.float32),
    ]
    in_specs = [per_tile(width, TILE), whole(*k.shape), whole(*v.shape)]
    scratch = [pltpu.VMEM((PAIRS, PAIR, 2 * TILE), jnp.bfloat16)]
    if first:
        out_specs, out_shape, extra = state_specs, state_shapes, ()
    else:
        in_specs = in_specs + state_specs
        out_specs = [per_tile(width, TILE), per_tile(2, PAIRS, 2 * TILE)]
        out_shape = [
            jax.ShapeDtypeStruct((tiles, width, TILE), jnp.bfloat16),
            jax.ShapeDtypeStruct((tiles, 2, PAIRS, 2 * TILE), jnp.float32),
        ]
        scratch = scratch + [pltpu.VMEM((1,) + s.shape[1:], s.dtype) for s in state_shapes]
        extra = tuple(state)
    pairs = tiles * 2
    return pl.pallas_call(
        functools.partial(attend_kernel, first, key_tiles),
        grid_spec=pltpu.PrefetchScalarGridSpec(
            num_scalar_prefetch=1, grid=(tiles,), in_specs=in_specs, out_specs=out_specs, scratch_shapes=scratch
        ),
        out_shape=out_shape,
        compiler_params=pltpu.CompilerParams(vmem_limit_bytes=VMEM_LIMIT),
        cost_estimate=pl.CostEstimate(
            flops=8 * pairs * TILE * TILE * width, bytes_accessed=4 * k.size, transcendentals=pairs * HEADS * TILE * TILE
        ),
        name="attend_near" if first else "attend_far",
    )(flags, q, k, v, *extra)


def finish_kernel(count, *refs):
    x_ref, wo_ref = refs[:2]
    parts, stats = refs[2 : 2 + count], refs[2 + count : 2 + 2 * count]
    out_ref, joined = refs[2 + 2 * count :]
    highest = stats[0][0, 0]
    for s in stats[1:]:
        highest = jnp.maximum(highest, s[0, 0])
    shares = [jnp.exp(s[0, 0] - highest) * s[0, 1] for s in stats]
    total = functools.reduce(lambda a, b: a + b, shares)
    shares = [s / total for s in shares]
    for h in range(HEADS):
        half = slice((h % 2) * TILE, (h % 2 + 1) * TILE)
        at = h * HEAD_DIM
        summed = sum(
            part[0, at : at + HEAD_DIM, :].astype(jnp.float32) * share[h // 2 : h // 2 + 1, half]
            for part, share in zip(parts, shares)
        )
        joined[at : at + HEAD_DIM, :] = summed.astype(jnp.bfloat16)
    added = lax.dot_general(
        joined[...], wo_ref[...], (((0,), (0,)), ((), ())), preferred_element_type=jnp.float32
    )
    out_ref[...] = (x_ref[...].astype(jnp.float32) + added).astype(jnp.bfloat16)


def finish(x, wo, parts, stats):
    rows, width = x.shape
    count = len(parts)
    return pl.pallas_call(
        functools.partial(finish_kernel, count),
        grid=(rows // TILE,),
        in_specs=[pl.BlockSpec((TILE, width), lambda i: (i, 0)), pl.BlockSpec((width, width), lambda i: (0, 0))]
        + [pl.BlockSpec((1, width, TILE), lambda i: (i, 0, 0))] * count
        + [pl.BlockSpec((1, 2, PAIRS, 2 * TILE), lambda i: (i, 0, 0, 0))] * count,
        out_specs=pl.BlockSpec((TILE, width), lambda i: (i, 0)),
        out_shape=jax.ShapeDtypeStruct((rows, width), jnp.bfloat16),
        scratch_shapes=[pltpu.VMEM((width, TILE), jnp.bfloat16)],
        compiler_params=pltpu.CompilerParams(vmem_limit_bytes=VMEM_LIMIT),
        name="finish",
    )(x, wo, *parts, *stats)


def shards(nodes, project_in, project_out, tile_list, tile_count):
    rows, width = nodes.shape
    groups, sp = lax.axis_size("pb"), lax.axis_size("sp")
    g, s = lax.axis_index("pb"), lax.axis_index("sp")
    own = rows // TILE
    group_tiles = own * sp
    far = lax.all_gather(nodes, "pb", axis=0, tiled=True)

    def swap(k, value):
        if k == 0:
            return value
        return lax.ppermute(value, "sp", [(i, i ^ k) for i in range(sp)])

    weights = project_in.T.reshape(HEADS, 3, HEAD_DIM, width).transpose(1, 0, 2, 3).reshape(3, width, width)
    wq, wk, wv = weights[0], weights[1], weights[2]
    q_own = project_query(nodes, wq)
    q = jnp.concatenate([swap(k, q_own) for k in range(sp)], axis=0)
    k_own, v_own = project_key_value(nodes, wk, wv, rows)

    partner = s ^ jnp.arange(sp, dtype=jnp.int32)
    local = jnp.arange(own, dtype=jnp.int32)
    q_tiles = (g * group_tiles + partner[:, None] * own + local[None, :]).reshape(-1)
    lists, counts = tile_list[q_tiles], tile_count[q_tiles]
    lists = jnp.where(jnp.arange(lists.shape[1], dtype=jnp.int32)[None, :] < counts[:, None], lists, -1)
    group_ids = jnp.arange(groups, dtype=jnp.int32)
    key_tiles = (group_ids[:, None] * group_tiles + s * own + local[None, :]).reshape(-1)
    used = jnp.any(lists[:, :, None] == key_tiles[None, None, :], axis=1).astype(jnp.int32)
    near = jnp.any(lists[:, :, None] == (g * group_tiles + s * own + local)[None, None, :], axis=1).astype(jnp.int32)
    distant = jnp.where((key_tiles // group_tiles == g)[None, :], 0, used)

    state = attend(near.reshape(-1), q, k_own, v_own)
    k_far, v_far = project_key_value(far, wk, wv, rows)
    part, stat = attend(distant.reshape(-1), q, k_far, v_far, state)
    parts = [swap(k, part[k * own : (k + 1) * own]) for k in range(sp)]
    stats = [swap(k, stat[k * own : (k + 1) * own]) for k in range(sp)]
    return finish(nodes, project_out, parts, stats)


def solution(mesh):
    in_specs = (P(("pb", "sp"), None), P(), P(), P(), P())
    out_specs = P(("pb", "sp"), None)
    return jax.shard_map(shards, mesh=mesh, in_specs=in_specs, out_specs=out_specs, check_vma=False)
```

```python
import functools

import jax
import jax.numpy as jnp
from jax import lax
from jax.experimental import pallas as pl
from jax.experimental.pallas import tpu as pltpu
from jax.sharding import PartitionSpec as P

HEADS = 16
HEAD_DIM = 64
TILE = 128
PAIR = 2 * HEAD_DIM
PAIRS = HEADS // 2
NEGATIVE = -1e30
TRANSPOSED = (((1,), (1,)), ((), ()))
MIB = 1024 * 1024
VMEM_LIMIT = 20 * MIB


def own_kernel(x_ref, w_ref, q_ref, k_ref, v_ref):
    y = jnp.dot(x_ref[...], w_ref[...], preferred_element_type=jnp.float32)
    turned = y.T
    e = HEAD_DIM
    q = jnp.concatenate([turned[:e], turned[3 * e : 4 * e]], axis=0).astype(jnp.bfloat16)
    q = q * jnp.bfloat16(HEAD_DIM ** -0.5)
    k = jnp.concatenate([turned[e : 2 * e], turned[4 * e : 5 * e]], axis=0)
    v = jnp.concatenate([turned[2 * e : 3 * e], turned[5 * e :]], axis=0).astype(jnp.bfloat16)
    k_ref[...] = k.T.astype(jnp.bfloat16)
    for j in range(q_ref.shape[0]):
        q_ref[j] = q[:, j * TILE : (j + 1) * TILE]
        v_ref[j] = v[:, j * TILE : (j + 1) * TILE]


def key_value_kernel(x_ref, wk_ref, wv_ref, k_ref, v_ref):
    x = x_ref[...]
    k = lax.dot_general(x, wk_ref[...], TRANSPOSED, preferred_element_type=jnp.float32)
    v = lax.dot_general(wv_ref[...], x, TRANSPOSED, preferred_element_type=jnp.float32)
    k_ref[...] = k.astype(jnp.bfloat16)
    v = v.astype(jnp.bfloat16)
    for j in range(v_ref.shape[0]):
        v_ref[j] = v[:, j * TILE : (j + 1) * TILE]


def project_own(x, w):
    rows, width = x.shape
    turned = jax.ShapeDtypeStruct((rows // TILE, width, TILE), jnp.bfloat16)
    turned_spec = pl.BlockSpec((rows // TILE, PAIR, TILE), lambda p: (0, p, 0))
    return pl.pallas_call(
        own_kernel,
        grid=(PAIRS,),
        in_specs=[
            pl.BlockSpec((rows, width), lambda p: (0, 0)),
            pl.BlockSpec((width, 3 * PAIR), lambda p: (0, p)),
        ],
        out_specs=[turned_spec, pl.BlockSpec((rows, PAIR), lambda p: (0, p)), turned_spec],
        out_shape=[turned, jax.ShapeDtypeStruct((rows, width), jnp.bfloat16), turned],
        compiler_params=pltpu.CompilerParams(vmem_limit_bytes=16 * 1024 * 1024),
        cost_estimate=pl.CostEstimate(flops=6 * rows * width * width, bytes_accessed=6 * width * width, transcendentals=0),
        name="own",
    )(x, w)


def project_key_value(x, wk, wv, step):
    rows, width = x.shape
    return pl.pallas_call(
        key_value_kernel,
        grid=(rows // step,),
        in_specs=[
            pl.BlockSpec((step, width), lambda i: (i, 0)),
            pl.BlockSpec((width, width), lambda i: (0, 0)),
            pl.BlockSpec((width, width), lambda i: (0, 0)),
        ],
        out_specs=[
            pl.BlockSpec((step, width), lambda i: (i, 0)),
            pl.BlockSpec((step // TILE, width, TILE), lambda i: (i, 0, 0)),
        ],
        out_shape=[
            jax.ShapeDtypeStruct((rows, width), jnp.bfloat16),
            jax.ShapeDtypeStruct((rows // TILE, width, TILE), jnp.bfloat16),
        ],
        compiler_params=pltpu.CompilerParams(vmem_limit_bytes=VMEM_LIMIT),
        cost_estimate=pl.CostEstimate(
            flops=4 * rows * width * width, bytes_accessed=6 * rows * width + 4 * width * width, transcendentals=0
        ),
        name="key_value",
    )(x, wk, wv)


def attend_kernel(first, offset, key_tiles, flags, q_ref, k_ref, v_ref, *rest):
    if first:
        acc_ref, m_ref, l_ref, spread = rest
    else:
        acc_in, m_in, l_in, out_ref, stat_ref, spread, acc_ref, m_ref, l_ref = rest
    tile = pl.program_id(0)

    @pl.when(tile == 0)
    def _():
        spread[...] = jnp.zeros_like(spread)

    for p in range(PAIRS):
        low = p * PAIR
        spread[p, :HEAD_DIM, :TILE] = q_ref[0, low : low + HEAD_DIM, :]
        spread[p, HEAD_DIM:, TILE:] = q_ref[0, low + HEAD_DIM : low + PAIR, :]
    if first:
        acc_ref[...] = jnp.zeros_like(acc_ref)
        m_ref[...] = jnp.full_like(m_ref, NEGATIVE)
        l_ref[...] = jnp.zeros_like(l_ref)
    else:
        acc_ref[...] = acc_in[...]
        m_ref[...] = m_in[...]
        l_ref[...] = l_in[...]

    def visit(kt, carry):
        @pl.when(flags[(tile + offset) * key_tiles + kt] > 0)
        def _():
            rows = pl.ds(pl.multiple_of(kt * TILE, TILE), TILE)
            for p in range(PAIRS):
                low = p * PAIR
                s = jnp.dot(k_ref[rows, low : low + PAIR], spread[p], preferred_element_type=jnp.float32)
                m_old = m_ref[0, p : p + 1, :]
                m_new = jnp.maximum(m_old, jnp.max(s, axis=0, keepdims=True))
                fade = jnp.exp(m_old - m_new)
                w = jnp.exp(s - m_new)
                m_ref[0, p : p + 1, :] = m_new
                l_ref[0, p : p + 1, :] = l_ref[0, p : p + 1, :] * fade + jnp.sum(w, axis=0, keepdims=True)
                w = w.astype(jnp.bfloat16)
                for i in range(2):
                    at = low + i * HEAD_DIM
                    half = slice(i * TILE, (i + 1) * TILE)
                    o = jnp.dot(v_ref[kt, at : at + HEAD_DIM, :], w[:, half], preferred_element_type=jnp.float32)
                    acc_ref[0, at : at + HEAD_DIM, :] = acc_ref[0, at : at + HEAD_DIM, :] * fade[:, half] + o

        return carry

    lax.fori_loop(0, key_tiles, visit, 0)
    if not first:
        total = l_ref[0]
        inverse = jnp.where(total > 0.0, 1.0 / jnp.where(total > 0.0, total, 1.0), 0.0)
        for h in range(HEADS):
            half = slice((h % 2) * TILE, (h % 2 + 1) * TILE)
            at = h * HEAD_DIM
            scaled = acc_ref[0, at : at + HEAD_DIM, :] * inverse[h // 2 : h // 2 + 1, half]
            out_ref[0, at : at + HEAD_DIM, :] = scaled.astype(jnp.bfloat16)
        stat_ref[0, 0] = m_ref[0]
        stat_ref[0, 1] = total


def attend(flags, offset, q, k, v, state=None):
    tiles, width, _ = q.shape
    key_tiles = v.shape[0]
    first = state is None
    per_tile = lambda *shape: pl.BlockSpec((1,) + shape, lambda t, f: (t,) + (0,) * len(shape))
    whole = lambda *shape: pl.BlockSpec(shape, lambda t, f: (0,) * len(shape))
    state_specs = [per_tile(width, TILE), per_tile(PAIRS, 2 * TILE), per_tile(PAIRS, 2 * TILE)]
    state_shapes = [
        jax.ShapeDtypeStruct((tiles, width, TILE), jnp.float32),
        jax.ShapeDtypeStruct((tiles, PAIRS, 2 * TILE), jnp.float32),
        jax.ShapeDtypeStruct((tiles, PAIRS, 2 * TILE), jnp.float32),
    ]
    in_specs = [per_tile(width, TILE), whole(*k.shape), whole(*v.shape)]
    scratch = [pltpu.VMEM((PAIRS, PAIR, 2 * TILE), jnp.bfloat16)]
    if first:
        out_specs, out_shape, extra = state_specs, state_shapes, ()
    else:
        in_specs = in_specs + state_specs
        out_specs = [per_tile(width, TILE), per_tile(2, PAIRS, 2 * TILE)]
        out_shape = [
            jax.ShapeDtypeStruct((tiles, width, TILE), jnp.bfloat16),
            jax.ShapeDtypeStruct((tiles, 2, PAIRS, 2 * TILE), jnp.float32),
        ]
        scratch = scratch + [pltpu.VMEM((1,) + s.shape[1:], s.dtype) for s in state_shapes]
        extra = tuple(state)
    pairs = tiles * 2
    return pl.pallas_call(
        functools.partial(attend_kernel, first, offset, key_tiles),
        grid_spec=pltpu.PrefetchScalarGridSpec(
            num_scalar_prefetch=1, grid=(tiles,), in_specs=in_specs, out_specs=out_specs, scratch_shapes=scratch
        ),
        out_shape=out_shape,
        compiler_params=pltpu.CompilerParams(vmem_limit_bytes=4 * (k.size + v.size) + 8 * MIB),
        cost_estimate=pl.CostEstimate(
            flops=8 * pairs * TILE * TILE * width, bytes_accessed=4 * k.size, transcendentals=pairs * HEADS * TILE * TILE
        ),
        name="attend_near" if first else "attend_far",
    )(flags, q, k, v, *extra)


def finish_kernel(count, *refs):
    x_ref, wo_ref = refs[:2]
    parts, stats = refs[2 : 2 + count], refs[2 + count : 2 + 2 * count]
    out_ref, joined = refs[2 + 2 * count :]
    highest = stats[0][0, 0]
    for s in stats[1:]:
        highest = jnp.maximum(highest, s[0, 0])
    shares = [jnp.exp(s[0, 0] - highest) * s[0, 1] for s in stats]
    total = functools.reduce(lambda a, b: a + b, shares)
    shares = [s / total for s in shares]
    for h in range(HEADS):
        half = slice((h % 2) * TILE, (h % 2 + 1) * TILE)
        at = h * HEAD_DIM
        summed = sum(
            part[0, at : at + HEAD_DIM, :].astype(jnp.float32) * share[h // 2 : h // 2 + 1, half]
            for part, share in zip(parts, shares)
        )
        joined[at : at + HEAD_DIM, :] = summed.astype(jnp.bfloat16)
    added = lax.dot_general(
        joined[...], wo_ref[...], (((0,), (0,)), ((), ())), preferred_element_type=jnp.float32
    )
    out_ref[...] = (x_ref[...].astype(jnp.float32) + added).astype(jnp.bfloat16)


def finish(x, wo, parts, stats):
    rows, width = x.shape
    count = len(parts)
    return pl.pallas_call(
        functools.partial(finish_kernel, count),
        grid=(rows // TILE,),
        in_specs=[pl.BlockSpec((TILE, width), lambda i: (i, 0)), pl.BlockSpec((width, width), lambda i: (0, 0))]
        + [pl.BlockSpec((1, width, TILE), lambda i: (i, 0, 0))] * count
        + [pl.BlockSpec((1, 2, PAIRS, 2 * TILE), lambda i: (i, 0, 0, 0))] * count,
        out_specs=pl.BlockSpec((TILE, width), lambda i: (i, 0)),
        out_shape=jax.ShapeDtypeStruct((rows, width), jnp.bfloat16),
        scratch_shapes=[pltpu.VMEM((width, TILE), jnp.bfloat16)],
        compiler_params=pltpu.CompilerParams(vmem_limit_bytes=VMEM_LIMIT),
        name="finish",
    )(x, wo, *parts, *stats)


def shards(nodes, project_in, project_out, tile_list, tile_count):
    rows, width = nodes.shape
    groups, sp = lax.axis_size("pb"), lax.axis_size("sp")
    g, s = lax.axis_index("pb"), lax.axis_index("sp")
    own = rows // TILE
    group_tiles = own * sp
    far = lax.all_gather(nodes, "pb", axis=0, tiled=True)

    def swap(k, value):
        if k == 0:
            return value
        return lax.ppermute(value, "sp", [(i, i ^ k) for i in range(sp)])

    q_own, k_own, v_own = project_own(nodes, project_in)
    queries = [swap(k, q_own) for k in range(sp)]
    weights = project_in.T.reshape(HEADS, 3, HEAD_DIM, width)
    wk, wv = weights[:, 1].reshape(width, width), weights[:, 2].reshape(width, width)

    partner = s ^ jnp.arange(sp, dtype=jnp.int32)
    local = jnp.arange(own, dtype=jnp.int32)
    q_tiles = (g * group_tiles + partner[:, None] * own + local[None, :]).reshape(-1)
    lists, counts = tile_list[q_tiles], tile_count[q_tiles]
    lists = jnp.where(jnp.arange(lists.shape[1], dtype=jnp.int32)[None, :] < counts[:, None], lists, -1)
    group_ids = jnp.arange(groups, dtype=jnp.int32)
    key_tiles = (group_ids[:, None] * group_tiles + s * own + local[None, :]).reshape(-1)
    used = jnp.any(lists[:, :, None] == key_tiles[None, None, :], axis=1).astype(jnp.int32)
    near = jnp.any(lists[:, :, None] == (g * group_tiles + s * own + local)[None, None, :], axis=1).astype(jnp.int32)
    distant = jnp.where((key_tiles // group_tiles == g)[None, :], 0, used)

    near, distant = near.reshape(-1), distant.reshape(-1)
    states = [attend(near, k * own, queries[k], k_own, v_own) for k in range(sp)]
    k_far, v_far = project_key_value(far, wk, wv, rows)
    parts, stats = [None] * sp, [None] * sp
    for k in reversed(range(sp)):
        part, stat = attend(distant, k * own, queries[k], k_far, v_far, states[k])
        parts[k], stats[k] = swap(k, part), swap(k, stat)
    return finish(nodes, project_out, parts, stats)


def solution(mesh):
    in_specs = (P(("pb", "sp"), None), P(), P(), P(), P())
    out_specs = P(("pb", "sp"), None)
    return jax.shard_map(shards, mesh=mesh, in_specs=in_specs, out_specs=out_specs, check_vma=False)
```

```python
import functools

import jax
import jax.numpy as jnp
from jax import lax
from jax.experimental import pallas as pl
from jax.experimental.pallas import tpu as pltpu
from jax.sharding import PartitionSpec as P

HEADS = 16
HEAD_DIM = 64
TILE = 128
PAIR = 2 * HEAD_DIM
PAIRS = HEADS // 2
NEGATIVE = -1e30
TRANSPOSED = (((1,), (1,)), ((), ()))
MIB = 1024 * 1024
VMEM_LIMIT = 20 * MIB


def own_kernel(x_ref, w_ref, q_ref, k_ref, v_ref, wk_ref, wv_ref):
    y = jnp.dot(x_ref[...], w_ref[...], preferred_element_type=jnp.float32)
    turned = y.T
    e = HEAD_DIM
    w = w_ref[...].T
    for i in range(2):
        at = 3 * e * i
        wk_ref[i * e : (i + 1) * e, :] = w[at + e : at + 2 * e]
        wv_ref[i * e : (i + 1) * e, :] = w[at + 2 * e : at + 3 * e]
    q = jnp.concatenate([turned[:e], turned[3 * e : 4 * e]], axis=0).astype(jnp.bfloat16)
    q = q * jnp.bfloat16(HEAD_DIM ** -0.5)
    k = jnp.concatenate([turned[e : 2 * e], turned[4 * e : 5 * e]], axis=0)
    v = jnp.concatenate([turned[2 * e : 3 * e], turned[5 * e :]], axis=0).astype(jnp.bfloat16)
    k_ref[...] = k.T.astype(jnp.bfloat16)
    for j in range(q_ref.shape[0]):
        q_ref[j] = q[:, j * TILE : (j + 1) * TILE]
        v_ref[j] = v[:, j * TILE : (j + 1) * TILE]


def key_value_kernel(skip, x_ref, wk_ref, wv_ref, k_ref, v_ref):
    x = x_ref[...]
    k = lax.dot_general(x, wk_ref[...], TRANSPOSED, preferred_element_type=jnp.float32)
    v = lax.dot_general(wv_ref[...], x, TRANSPOSED, preferred_element_type=jnp.float32)
    k_ref[...] = k.astype(jnp.bfloat16)
    v = v.astype(jnp.bfloat16)
    for j in range(v_ref.shape[0]):
        v_ref[j] = v[:, j * TILE : (j + 1) * TILE]


def project_own(x, w):
    rows, width = x.shape
    turned = jax.ShapeDtypeStruct((rows // TILE, width, TILE), jnp.bfloat16)
    turned_spec = pl.BlockSpec((rows // TILE, PAIR, TILE), lambda p: (0, p, 0))
    return pl.pallas_call(
        own_kernel,
        grid=(PAIRS,),
        in_specs=[
            pl.BlockSpec((rows, width), lambda p: (0, 0)),
            pl.BlockSpec((width, 3 * PAIR), lambda p: (0, p)),
        ],
        out_specs=[turned_spec, pl.BlockSpec((rows, PAIR), lambda p: (0, p)), turned_spec]
        + [pl.BlockSpec((PAIR, width), lambda p: (p, 0))] * 2,
        out_shape=[turned, jax.ShapeDtypeStruct((rows, width), jnp.bfloat16), turned]
        + [jax.ShapeDtypeStruct((width, width), jnp.bfloat16)] * 2,
        compiler_params=pltpu.CompilerParams(vmem_limit_bytes=16 * 1024 * 1024),
        cost_estimate=pl.CostEstimate(flops=6 * rows * width * width, bytes_accessed=6 * width * width, transcendentals=0),
        name="own",
    )(x, w)


def project_key_value(skip, x, wk, wv, step):
    rows, width = x.shape
    return pl.pallas_call(
        key_value_kernel,
        grid_spec=pltpu.PrefetchScalarGridSpec(
            num_scalar_prefetch=1,
            grid=(rows // step - 1,),
            in_specs=[
                pl.BlockSpec((step, width), lambda i, g: (i + (i >= g[0]).astype(jnp.int32), 0)),
                pl.BlockSpec((width, width), lambda i, g: (0, 0)),
                pl.BlockSpec((width, width), lambda i, g: (0, 0)),
            ],
            out_specs=[
                pl.BlockSpec((step, width), lambda i, g: (i + (i >= g[0]).astype(jnp.int32), 0)),
                pl.BlockSpec((step // TILE, width, TILE), lambda i, g: (i + (i >= g[0]).astype(jnp.int32), 0, 0)),
            ],
        ),
        out_shape=[
            jax.ShapeDtypeStruct((rows, width), jnp.bfloat16),
            jax.ShapeDtypeStruct((rows // TILE, width, TILE), jnp.bfloat16),
        ],
        compiler_params=pltpu.CompilerParams(vmem_limit_bytes=VMEM_LIMIT),
        cost_estimate=pl.CostEstimate(
            flops=4 * rows * width * width, bytes_accessed=6 * rows * width + 4 * width * width, transcendentals=0
        ),
        name="key_value",
    )(skip, x, wk, wv)


def attend_kernel(first, offset, key_tiles, flags, q_ref, k_ref, v_ref, *rest):
    if first:
        acc_ref, m_ref, l_ref, spread = rest
    else:
        acc_in, m_in, l_in, out_ref, stat_ref, spread, acc_ref, m_ref, l_ref = rest
    tile = pl.program_id(0)

    @pl.when(tile == 0)
    def _():
        spread[...] = jnp.zeros_like(spread)

    for p in range(PAIRS):
        low = p * PAIR
        spread[p, :HEAD_DIM, :TILE] = q_ref[0, low : low + HEAD_DIM, :]
        spread[p, HEAD_DIM:, TILE:] = q_ref[0, low + HEAD_DIM : low + PAIR, :]
    if first:
        acc_ref[...] = jnp.zeros_like(acc_ref)
        m_ref[...] = jnp.full_like(m_ref, NEGATIVE)
        l_ref[...] = jnp.zeros_like(l_ref)
    else:
        acc_ref[...] = acc_in[...]
        m_ref[...] = m_in[...]
        l_ref[...] = l_in[...]

    def visit(kt, carry):
        @pl.when(flags[(tile + offset) * key_tiles + kt] > 0)
        def _():
            rows = pl.ds(pl.multiple_of(kt * TILE, TILE), TILE)
            for p in range(PAIRS):
                low = p * PAIR
                s = jnp.dot(k_ref[rows, low : low + PAIR], spread[p], preferred_element_type=jnp.float32)
                m_old = m_ref[0, p : p + 1, :]
                m_new = jnp.maximum(m_old, jnp.max(s, axis=0, keepdims=True))
                fade = jnp.exp(m_old - m_new)
                w = jnp.exp(s - m_new)
                m_ref[0, p : p + 1, :] = m_new
                l_ref[0, p : p + 1, :] = l_ref[0, p : p + 1, :] * fade + jnp.sum(w, axis=0, keepdims=True)
                w = w.astype(jnp.bfloat16)
                for i in range(2):
                    at = low + i * HEAD_DIM
                    half = slice(i * TILE, (i + 1) * TILE)
                    o = jnp.dot(v_ref[kt, at : at + HEAD_DIM, :], w[:, half], preferred_element_type=jnp.float32)
                    acc_ref[0, at : at + HEAD_DIM, :] = acc_ref[0, at : at + HEAD_DIM, :] * fade[:, half] + o

        return carry

    lax.fori_loop(0, key_tiles, visit, 0)
    if not first:
        total = l_ref[0]
        inverse = jnp.where(total > 0.0, 1.0 / jnp.where(total > 0.0, total, 1.0), 0.0)
        for h in range(HEADS):
            half = slice((h % 2) * TILE, (h % 2 + 1) * TILE)
            at = h * HEAD_DIM
            scaled = acc_ref[0, at : at + HEAD_DIM, :] * inverse[h // 2 : h // 2 + 1, half]
            out_ref[0, at : at + HEAD_DIM, :] = scaled.astype(jnp.bfloat16)
        stat_ref[0, 0] = m_ref[0]
        stat_ref[0, 1] = total


def attend(flags, offset, q, k, v, state=None):
    tiles, width, _ = q.shape
    key_tiles = v.shape[0]
    first = state is None
    per_tile = lambda *shape: pl.BlockSpec((1,) + shape, lambda t, f: (t,) + (0,) * len(shape))
    whole = lambda *shape: pl.BlockSpec(shape, lambda t, f: (0,) * len(shape))
    state_specs = [per_tile(width, TILE), per_tile(PAIRS, 2 * TILE), per_tile(PAIRS, 2 * TILE)]
    state_shapes = [
        jax.ShapeDtypeStruct((tiles, width, TILE), jnp.float32),
        jax.ShapeDtypeStruct((tiles, PAIRS, 2 * TILE), jnp.float32),
        jax.ShapeDtypeStruct((tiles, PAIRS, 2 * TILE), jnp.float32),
    ]
    in_specs = [per_tile(width, TILE), whole(*k.shape), whole(*v.shape)]
    scratch = [pltpu.VMEM((PAIRS, PAIR, 2 * TILE), jnp.bfloat16)]
    if first:
        out_specs, out_shape, extra = state_specs, state_shapes, ()
    else:
        in_specs = in_specs + state_specs
        out_specs = [per_tile(width, TILE), per_tile(2, PAIRS, 2 * TILE)]
        out_shape = [
            jax.ShapeDtypeStruct((tiles, width, TILE), jnp.bfloat16),
            jax.ShapeDtypeStruct((tiles, 2, PAIRS, 2 * TILE), jnp.float32),
        ]
        scratch = scratch + [pltpu.VMEM((1,) + s.shape[1:], s.dtype) for s in state_shapes]
        extra = tuple(state)
    pairs = tiles * 2
    return pl.pallas_call(
        functools.partial(attend_kernel, first, offset, key_tiles),
        grid_spec=pltpu.PrefetchScalarGridSpec(
            num_scalar_prefetch=1, grid=(tiles,), in_specs=in_specs, out_specs=out_specs, scratch_shapes=scratch
        ),
        out_shape=out_shape,
        compiler_params=pltpu.CompilerParams(vmem_limit_bytes=4 * (k.size + v.size) + 8 * MIB),
        cost_estimate=pl.CostEstimate(
            flops=8 * pairs * TILE * TILE * width, bytes_accessed=4 * k.size, transcendentals=pairs * HEADS * TILE * TILE
        ),
        name="attend_near" if first else "attend_far",
    )(flags, q, k, v, *extra)


def finish_kernel(count, *refs):
    x_ref, wo_ref = refs[:2]
    parts, stats = refs[2 : 2 + count], refs[2 + count : 2 + 2 * count]
    out_ref, joined = refs[2 + 2 * count :]
    highest = stats[0][0, 0]
    for s in stats[1:]:
        highest = jnp.maximum(highest, s[0, 0])
    shares = [jnp.exp(s[0, 0] - highest) * s[0, 1] for s in stats]
    total = functools.reduce(lambda a, b: a + b, shares)
    shares = [s / total for s in shares]
    for h in range(HEADS):
        half = slice((h % 2) * TILE, (h % 2 + 1) * TILE)
        at = h * HEAD_DIM
        summed = sum(
            part[0, at : at + HEAD_DIM, :].astype(jnp.float32) * share[h // 2 : h // 2 + 1, half]
            for part, share in zip(parts, shares)
        )
        joined[at : at + HEAD_DIM, :] = summed.astype(jnp.bfloat16)
    added = lax.dot_general(
        joined[...], wo_ref[...], (((0,), (0,)), ((), ())), preferred_element_type=jnp.float32
    )
    out_ref[...] = (x_ref[...].astype(jnp.float32) + added).astype(jnp.bfloat16)


def finish(x, wo, parts, stats):
    rows, width = x.shape
    count = len(parts)
    return pl.pallas_call(
        functools.partial(finish_kernel, count),
        grid=(rows // TILE,),
        in_specs=[pl.BlockSpec((TILE, width), lambda i: (i, 0)), pl.BlockSpec((width, width), lambda i: (0, 0))]
        + [pl.BlockSpec((1, width, TILE), lambda i: (i, 0, 0))] * count
        + [pl.BlockSpec((1, 2, PAIRS, 2 * TILE), lambda i: (i, 0, 0, 0))] * count,
        out_specs=pl.BlockSpec((TILE, width), lambda i: (i, 0)),
        out_shape=jax.ShapeDtypeStruct((rows, width), jnp.bfloat16),
        scratch_shapes=[pltpu.VMEM((width, TILE), jnp.bfloat16)],
        compiler_params=pltpu.CompilerParams(vmem_limit_bytes=VMEM_LIMIT),
        name="finish",
    )(x, wo, *parts, *stats)


def shards(nodes, project_in, project_out, tile_list, tile_count):
    rows, width = nodes.shape
    groups, sp = lax.axis_size("pb"), lax.axis_size("sp")
    g, s = lax.axis_index("pb"), lax.axis_index("sp")
    own = rows // TILE
    group_tiles = own * sp
    far = lax.all_gather(nodes, "pb", axis=0, tiled=True)

    def swap(k, value):
        if k == 0:
            return value
        return lax.ppermute(value, "sp", [(i, i ^ k) for i in range(sp)])

    q_own, k_own, v_own, wk, wv = project_own(nodes, project_in)
    queries = [swap(k, q_own) for k in range(sp)]
    partner = s ^ jnp.arange(sp, dtype=jnp.int32)
    local = jnp.arange(own, dtype=jnp.int32)
    q_tiles = (g * group_tiles + partner[:, None] * own + local[None, :]).reshape(-1)
    lists, counts = tile_list[q_tiles], tile_count[q_tiles]
    lists = jnp.where(jnp.arange(lists.shape[1], dtype=jnp.int32)[None, :] < counts[:, None], lists, -1)
    group_ids = jnp.arange(groups, dtype=jnp.int32)
    key_tiles = (group_ids[:, None] * group_tiles + s * own + local[None, :]).reshape(-1)
    used = jnp.any(lists[:, :, None] == key_tiles[None, None, :], axis=1).astype(jnp.int32)
    near = jnp.any(lists[:, :, None] == (g * group_tiles + s * own + local)[None, None, :], axis=1).astype(jnp.int32)
    distant = jnp.where((key_tiles // group_tiles == g)[None, :], 0, used)

    near, distant = near.reshape(-1), distant.reshape(-1)
    states = [attend(near, k * own, queries[k], k_own, v_own) for k in range(sp)]
    k_far, v_far = project_key_value(jnp.reshape(g, (1,)).astype(jnp.int32), far, wk, wv, rows)
    parts, stats = [None] * sp, [None] * sp
    for k in reversed(range(sp)):
        part, stat = attend(distant, k * own, queries[k], k_far, v_far, states[k])
        parts[k], stats[k] = swap(k, part), swap(k, stat)
    return finish(nodes, project_out, parts, stats)


def solution(mesh):
    in_specs = (P(("pb", "sp"), None), P(), P(), P(), P())
    out_specs = P(("pb", "sp"), None)
    return jax.shard_map(shards, mesh=mesh, in_specs=in_specs, out_specs=out_specs, check_vma=False)
```
